32 devices in a mesh: groups: 2 (over y), rows: 4 (over z), cols: 2 (over x), sub: 2 (over core).
Axes of the slice: x: 2, y: 2, z: 4, core: 2. Of those that a mesh axis runs over, the one named last changes fastest.
Arguments:
- tile_index: int32 [64, 2], P(('groups', 'rows', 'cols', 'sub')), parts along dimension 0, may hold values from 0 to 7, as said below
- tile_values: bfloat16 [64, 256, 256], P(('groups', 'rows', 'cols', 'sub')), parts along dimension 0, may hold values from -0.125 to 0.125
- onsite_energy: float32 [4096], P(('groups', 'rows', 'cols')), parts along dimension 0, may hold values from 0.5 to 4
- start_block: float32 [4096, 64], P(('groups', 'rows', 'cols')), parts along dimension 0, may hold values from -6 to 6
- previous_block: float32 [4096, 64], P(('groups', 'rows', 'cols')), parts along dimension 0, may hold values from -6 to 6
- previous_coupling: float32 [128, 64], P('groups'), parts along dimension 0, may hold values from -0.6 to 0.6
- stored_basis: float32 [8, 4096, 64], P('sub', ('groups', 'rows', 'cols')), parts along dimension 1, may hold values from -6 to 6
Outputs:
- new_blocks: float32 [1, 4096, 64], P(None, ('groups', 'rows', 'cols')), parts along dimension 1
- diagonal_blocks: float32 [1, 128, 64], P(None, 'groups'), parts along dimension 1
- coupling_blocks: float32 [1, 128, 64], P(None, 'groups'), parts along dimension 1
The draws below stay inside these ranges and needn't reach their ends.
There are 2 independent parts, one for each index of `groups`. The reference program is written for one: setup_inputs(seed, part) draws one part's arguments, and reference() takes and returns one part's arrays. A program takes and returns all parts, laid end to end along the dimension named above; each array names one. Nothing has to cross between parts.
Inputs may be any that keep to these rules, and one draw needn't show every extreme that they name: `tile_index`: tile rows of a device's tiles lie in the rows of the operator that the device's index of rows and cols holds; tile columns lie in the rows held by some index of rows with the same index of cols. Tiles may repeat.
All inputs are finite; a program needn't handle non-finite values.
Results may differ from the reference program's by a relative error of at most 0.0019.
Values may be sent and summed in bfloat16 or wider, within the bound.
A program may use at most 64 MiB of HBM per device.

```python
import math
import jax
import jax.numpy as jnp
from jax import lax

BLOCK = 64
TILE = 256
STORED = 8
ITERS = 1
TROWS_DEV = 1
TILES_DEV = 2
ORDER = 2048
TILES = 32
N_ROWS = 4
N_COLS = 2
N_SUB = 2


def draw_tile_index(key, part):
    count = TILES_DEV * N_ROWS * N_COLS * N_SUB
    device = jnp.arange(count, dtype=jnp.int32) // TILES_DEV
    own_slice = device // N_SUB
    own_column = own_slice % N_COLS
    first_key, second_key, third_key = jax.random.split(jax.random.fold_in(key, 17), 3)
    local_row = jax.random.randint(first_key, (count,), 0, TROWS_DEV)
    source_band = jax.random.randint(second_key, (count,), 0, N_ROWS)
    source_row = jax.random.randint(third_key, (count,), 0, TROWS_DEV)
    tile_row = own_slice * TROWS_DEV + local_row
    tile_column = (source_band * N_COLS + own_column) * TROWS_DEV + source_row
    return jnp.stack([tile_row, tile_column], axis=1).astype(jnp.int32)


def draw_stored_basis(key, part):
    subkeys = jax.random.split(jax.random.fold_in(key, 29), 3)
    private = jax.random.normal(subkeys[0], (STORED, ORDER, BLOCK), jnp.float32)
    common = jax.random.normal(subkeys[1], (ORDER, BLOCK), jnp.float32)
    mixing = jnp.eye(BLOCK, dtype=jnp.float32)[None] + 0.6 * jax.random.normal(subkeys[2], (STORED, BLOCK, BLOCK), jnp.float32) / jnp.sqrt(jnp.float32(BLOCK))
    blended = jnp.einsum('kib,kbc->kic', private, mixing, precision=lax.Precision.HIGHEST) * 0.857493
    values = 0.5 * blended + 0.866 * common[None]
    return jnp.clip(values, -6.0, 6.0).astype(jnp.float32)


def level_of(key, shape, cuts, low, largest):
    gain, own = 1.0, jax.random.fold_in(key, 6)
    for axis_at, shards_of in cuts:
        heights = jnp.exp(jax.random.uniform(jax.random.fold_in(own, axis_at), (shards_of,), jnp.float32, low / len(cuts), largest / len(cuts)))
        gain = gain * jnp.repeat(heights, shape[axis_at] // shards_of).reshape([-1 if axis == axis_at else 1 for axis in range(len(shape))])
    return gain


def gaussian(key, dims, deviation, limit, cuts=(), kind=jnp.bfloat16):
    loudness = level_of(key, dims, cuts, -0.22, 0.18) if cuts else 1.0
    result = jax.random.normal(key, dims, jnp.float32) * deviation * loudness
    return jnp.minimum(jnp.maximum(result, -limit), limit).astype(kind)


def setup_inputs(seed: int = 0, part: int = 0) -> dict:
    streams_of = jax.random.split(jax.random.key(seed), 8)
    own_keys = jax.random.split(jax.random.fold_in(streams_of[7], part), 8)
    tile_index = draw_tile_index(jax.random.fold_in(jax.random.fold_in(streams_of[7], part), 71), part)
    tile_values = gaussian(own_keys[1], (TILES, TILE, TILE), (4 * TILES_DEV * TILE // TROWS_DEV) ** -0.5, 0.125, ((0, 16),))
    onsite_energy = jnp.clip(jnp.exp(math.log(4.0) - 2.0794415 * jax.random.uniform(own_keys[2], (ORDER,), jnp.float32) ** level_of(own_keys[2], (ORDER,), ((0, 8),), -0.2, 0.2)), 0.5, 4.0)
    start_block = gaussian(own_keys[3], (ORDER, BLOCK), 1.0, 6.0, ((0, 8),), jnp.float32)
    previous_block = gaussian(own_keys[4], (ORDER, BLOCK), 1.0, 6.0, ((0, 8),), jnp.float32)
    previous_coupling = gaussian(own_keys[5], (BLOCK, BLOCK), 0.1, 0.6, (), jnp.float32)
    stored_basis = draw_stored_basis(jax.random.fold_in(jax.random.fold_in(streams_of[7], part), 71), part)
    return {"tile_index": tile_index, "tile_values": tile_values, "onsite_energy": onsite_energy, "start_block": start_block, "previous_block": previous_block, "previous_coupling": previous_coupling, "stored_basis": stored_basis}


highest = lax.Precision.HIGHEST

def apply_operator(tile_index, tile_values, onsite_energy, current):
    tile_rows = ORDER // TILE
    narrow = lax.optimization_barrier(current.astype(jnp.bfloat16))
    rounded = narrow.astype(jnp.float32).reshape(tile_rows, TILE, BLOCK)
    grouped_index = tile_index.reshape(-1, TILES_DEV, 2)
    grouped_values = tile_values.reshape(-1, TILES_DEV, TILE, TILE)

    def accumulate(total, item):
        indices, values = item
        values = values.astype(jnp.float32)
        pulled = jnp.einsum('kab,kbn->kan', values, rounded[indices[:, 1]], precision=highest)
        pushed = jnp.einsum('kab,kan->kbn', values, rounded[indices[:, 0]], precision=highest)
        total = total.at[indices[:, 0]].add(pulled)
        total = total.at[indices[:, 1]].add(pushed)
        return (total, None)
    initial = jnp.zeros((tile_rows, TILE, BLOCK), jnp.float32)
    total, unused = lax.scan(accumulate, initial, (grouped_index, grouped_values))
    return total.reshape(ORDER, BLOCK) + onsite_energy[:, None] * current

def reference(tile_index, tile_values, onsite_energy, start_block, previous_block, previous_coupling, stored_basis):
    current = start_block
    earlier = previous_block
    coupling = jnp.triu(previous_coupling)
    new_list = []
    diagonal_list = []
    coupling_list = []
    for iteration in range(ITERS):
        images = apply_operator(tile_index, tile_values, onsite_energy, current)
        images = images - jnp.dot(earlier, coupling.T, precision=highest)
        diagonal = jnp.dot(current.T, images, precision=highest) / ORDER
        images = images - jnp.dot(current, diagonal, precision=highest)
        projection = jnp.einsum('kib,ic->kbc', stored_basis, images, precision=highest) / ORDER
        images = images - jnp.einsum('kib,kbc->ic', stored_basis, projection, precision=highest)
        gram = jnp.dot(images.T, images, precision=highest) / ORDER
        lower_factor = jnp.linalg.cholesky(gram)
        following = lax.linalg.triangular_solve(lower_factor, images, left_side=False, lower=True, transpose_a=True)
        new_list.append(following)
        diagonal_list.append(diagonal)
        coupling_list.append(lower_factor.T)
        earlier = current
        coupling = lower_factor.T
        current = following
    return (jnp.stack(new_list), jnp.stack(diagonal_list), jnp.stack(coupling_list))
```

```python
import functools

import jax
import jax.numpy as jnp
from jax import lax
from jax.experimental import pallas as pl
from jax.experimental.pallas import tpu as pltpu
from jax.sharding import PartitionSpec as P

MESH = pl.DeviceIdType.MESH
NN = (((1,), (0,)), ((), ()))
NT = (((1,), (1,)), ((), ()))
CH = 16
LANES = 128


def split(x):
    high = x.astype(jnp.bfloat16)
    return high, (x - high.astype(jnp.float32)).astype(jnp.bfloat16)


def mm(a, b, dims):
    return lax.dot_general(a, b, dims, preferred_element_type=jnp.float32)


def dot3(a, b, dims):
    return mm(a[0], b[0], dims) + (mm(a[0], b[1], dims) + mm(a[1], b[0], dims))


def loop(lo, hi, body):
    if hi - lo <= 20:
        for i in range(lo, hi):
            body(i)
    else:
        lax.fori_loop(lo, hi, lambda i, c: (body(i), c)[1], 0)


def eliminate(full, block):
    count = block // 8
    parts = [full[8 * b:8 * b + 8] for b in range(count)]
    wide = (8, full.shape[1])
    sub_id = lax.broadcasted_iota(jnp.int32, wide, 0)
    done = []
    for b in range(count):
        rows = [jnp.broadcast_to(parts[b][p:p + 1], wide) for p in range(8)]
        cols = [
            [jnp.broadcast_to(parts[a][:, 8 * b + q:8 * b + q + 1], wide) for a in range(b, count)]
            for q in range(8)
        ]
        square = [[jnp.broadcast_to(cols[q][0][p:p + 1], wide) for q in range(8)] for p in range(8)]
        pivot = square[0][0]
        for p in range(8):
            inverse = 1.0 / square[p][p]
            for q in range(p + 1, 8):
                m = square[p][q] * inverse
                for t in range(q, 8):
                    square[q][t] = square[q][t] - m * square[p][t]
                rows[q] = rows[q] - m * rows[p]
            for i, a in enumerate(range(b, count)):
                factor = cols[p][i] * inverse
                if a == b:
                    factor = jnp.where(sub_id > p, factor, 0.0)
                for q in range(p + 1, 8):
                    cols[q][i] = cols[q][i] - factor * square[p][q]
                parts[a] = parts[a] - factor * rows[p]
            pivot = jnp.where(sub_id == p, square[p][p], pivot)
        done.append(parts[b] * lax.rsqrt(pivot))
    return jnp.concatenate(done, axis=0)


def kernel(
    dims, index_ref, tiles_in, onsite_ref, start_in, previous_in, coupling_ref, stored_in,
    image_ref, diag_ref, gram_ref,
    tiles_ref, start_ref, previous_ref, stored_ref, load_sem,
    gathered, terms, pushed_in, own_out, own_in, half_in,
    corr_snd, corr_rcv, corr_full, raw_snd, raw_rcv, raw_full,
    image_half, image_other, gram_rcv,
    x_send, x_recv, p_send, p_recv, pair_send, pair_recv,
    cs_send, cs_recv, cg_send, cg_recv, rs_send, rs_recv, rg_send, rg_recv, g_send, g_recv,
):
    R, C, S = dims
    n = R * C * S
    r, c, s = lax.axis_index("rows"), lax.axis_index("cols"), lax.axis_index("sub")
    me = (r * C + c) * S + s
    block, rows = start_ref.shape
    half = rows // 2
    count = tiles_ref.shape[0]
    mine_k = stored_ref.shape[0]
    total_rows = rows * R * C
    inv_n = 1.0 / total_rows

    def dev(p):
        return {"rows": p // (C * S), "cols": (p // S) % C, "sub": p % S}

    def remote(src, dst, send, recv, target):
        return pltpu.make_async_remote_copy(
            src_ref=src, dst_ref=dst, send_sem=send, recv_sem=recv,
            device_id=target, device_id_type=MESH,
        )

    partner = {"rows": r, "cols": c, "sub": 1 - s}
    barrier = pltpu.get_barrier_semaphore()

    def greet(i):
        pl.semaphore_signal(barrier, inc=1, device_id=dev(lax.rem(me + i, n)), device_id_type=MESH)

    loads = [
        pltpu.make_async_copy(src, dst, load_sem.at[i])
        for i, (src, dst) in enumerate((
            (start_in, start_ref), (tiles_in, tiles_ref), (stored_in, stored_ref), (previous_in, previous_ref),
        ))
    ]
    for load in loads:
        load.start()
    loop(1, n, greet)

    for load in loads:
        load.wait()
    xt = start_ref[...]
    pt = previous_ref[...]
    xb = xt.astype(jnp.bfloat16)
    gathered[r] = xb
    first = s == 0

    def pick(v):
        return jnp.where(first, v[:, :half], v[:, half:])

    def pick_other(v):
        return jnp.where(first, v[:, half:], v[:, :half])

    pushed = [mm(xb, tiles_ref[k], NN) for k in range(count)]
    bands = [index_ref[k, 1] // C for k in range(count)]

    def term(band):
        total = jnp.where(bands[0] == band, pushed[0], 0.0)
        for k in range(1, count):
            total = total + jnp.where(bands[k] == band, pushed[k], 0.0)
        return total

    def fill(i):
        band = lax.rem(r + i, R)
        value = term(band).astype(jnp.bfloat16)
        terms[i, 0] = value[:, :half]
        terms[i, 1] = value[:, half:]

    loop(1, R, fill)
    pl.semaphore_wait(barrier, n - 1)

    def x_copy(i):
        return remote(gathered.at[r], gathered.at[r], x_send.at[i], x_recv.at[r],
                      {"rows": lax.rem(r + i, R), "cols": c, "sub": s})

    def p_copy(i, j):
        return remote(terms.at[i, j], pushed_in.at[r, s], p_send.at[i, j], p_recv.at[r, s],
                      {"rows": lax.rem(r + i, R), "cols": c, "sub": j})

    far = pl.ds(pl.multiple_of((1 - s) * half, LANES), half)
    pair0 = remote(stored_ref.at[:, :, far], half_in, pair_send.at[0], pair_recv.at[0], partner)
    pair0.start()
    loop(1, R, lambda i: x_copy(i).start())

    def push(i):
        p_copy(i, 0).start()
        p_copy(i, 1).start()

    loop(1, R, push)

    own_half = pick(stored_ref[...].reshape(mine_k * block, rows))
    x_half = pick(xt)
    p_half = pick(pt)
    x_split = split(x_half)
    row_id = lax.broadcasted_iota(jnp.int32, (block, block), 0)
    col_id = lax.broadcasted_iota(jnp.int32, (block, block), 1)
    upper = jnp.where(col_id >= row_id, coupling_ref[...], 0.0)
    base = pick(onsite_ref[...]) * x_half - dot3(split(upper), split(p_half), NN)

    def exchange(nch, snd, rcv, full, ssend, srecv, gsend, grecv):
        slots = (nch + n - 1) // n

        def scatter():
            for t in range(slots):
                if (t + 1) * n <= nch:
                    rcv[t, me] = snd[t * n + me]

                    def send(i):
                        p = lax.rem(me + i, n)
                        remote(snd.at[t * n + p], rcv.at[t, me], ssend.at[t * n + p],
                               srecv.at[t, me], dev(p)).start()

                    loop(1, n, send)
                else:
                    for ch in range(t * n, nch):
                        p = ch - t * n

                        @pl.when(me == p)
                        def _():
                            rcv[t, p] = snd[ch]

                        @pl.when(me != p)
                        def _():
                            remote(snd.at[ch], rcv.at[t, me], ssend.at[ch],
                                   srecv.at[t, me], dev(p)).start()

        def owned(t):
            return nch - t * n if (t + 1) * n > nch else n

        def gather_copy(t, i):
            p = lax.rem(me + i, n)
            return remote(full.at[t * n + me], full.at[t * n + me], gsend.at[t, i],
                          grecv.at[t * n + me], dev(p))

        def reduce_and_gather():
            for t in range(slots):
                def run():
                    def wait(i):
                        p = lax.rem(me + n - i, n)
                        remote(snd.at[0], rcv.at[t, p], ssend.at[0], srecv.at[t, p], dev(p)).wait_recv()

                    loop(1, n, wait)
                    full[t * n + me] = jnp.sum(rcv[t].astype(jnp.float32), axis=0)
                    loop(1, n, lambda i: gather_copy(t, i).start())

                if owned(t) == n:
                    run()
                else:
                    pl.when(me < owned(t))(run)

        def finish():
            for t in range(slots):
                if owned(t) == n:
                    def wait(i):
                        p = lax.rem(me + n - i, n)
                        remote(full.at[t * n + p], full.at[t * n + p], gsend.at[t, 0],
                               grecv.at[t * n + p], dev(p)).wait_recv()

                    loop(1, n, wait)
                else:
                    for p in range(owned(t)):
                        @pl.when(me != p)
                        def _():
                            remote(full.at[t * n + p], full.at[t * n + p], gsend.at[t, 0],
                                   grecv.at[t * n + p], dev(p)).wait_recv()

        def drain():
            for t in range(slots):
                if owned(t) == n:
                    def wait(i):
                        p = lax.rem(me + i, n)
                        remote(snd.at[t * n + p], rcv.at[t, me], ssend.at[t * n + p],
                               srecv.at[t, me], dev(p)).wait_send()
                        gather_copy(t, i).wait_send()

                    loop(1, n, wait)
                else:
                    for p in range(owned(t)):
                        @pl.when(me != p)
                        def _():
                            remote(snd.at[t * n + p], rcv.at[t, me], ssend.at[t * n + p],
                                   srecv.at[t, me], dev(p)).wait_send()

                    @pl.when(me < owned(t))
                    def _():
                        loop(1, n, lambda i: gather_copy(t, i).wait_send())

        return scatter, reduce_and_gather, finish, drain

    per = block // CH
    corr_n = corr_snd.shape[0]
    raw_n = raw_snd.shape[0]
    wide = corr_n // per
    pack = (raw_n - corr_n) // 2

    def put(snd, value):
        for kt in range(wide):
            for q in range(per):
                snd[kt * per + q] = value[q * CH:(q + 1) * CH, kt * LANES:(kt + 1) * LANES].astype(snd.dtype)

    def take(full):
        parts = [jnp.concatenate([full[kt * per + q] for q in range(per)], axis=0) for kt in range(wide)]
        return jnp.concatenate(parts, axis=1)

    corr = exchange(corr_n, corr_snd, corr_rcv, corr_full, cs_send, cs_recv, cg_send, cg_recv)
    raw = exchange(raw_n, raw_snd, raw_rcv, raw_full, rs_send, rs_recv, rg_send, rg_recv)

    pair0.wait_recv()
    other_half = half_in[...].reshape(mine_k * block, half)
    both = jnp.concatenate([jnp.where(first, own_half, other_half), jnp.where(first, other_half, own_half)], axis=0)
    basis = split(both)
    put(corr_snd, dot3(x_split, basis, NT))
    corr[0]()

    def x_wait(i):
        p = lax.rem(r + R - i, R)
        remote(gathered.at[p], gathered.at[p], x_send.at[i], x_recv.at[p], partner).wait_recv()

    loop(1, R, x_wait)
    own = term(r)
    for k in range(count):
        own = own + mm(gathered[bands[k]], tiles_ref[k], NT)
    own_out[...] = pick_other(own)
    pair1 = remote(own_out, own_in, pair_send.at[1], pair_recv.at[1], partner)
    pair1.start()
    w = base + pick(own)

    def p_wait(i):
        p = lax.rem(r + R - i, R)
        for j in range(S):
            remote(terms.at[1, j], pushed_in.at[p, j], p_send.at[1, j], p_recv.at[p, j], partner).wait_recv()

    loop(1, R, p_wait)
    pushed_in[r] = jnp.zeros((S, block, half), jnp.bfloat16)
    received = jnp.sum(pushed_in[...].astype(jnp.float32), axis=(0, 1))
    pair1.wait_recv()
    w = w + (received + own_in[...])
    w_split = split(w)
    put(raw_snd, dot3(w_split, basis, NT))
    diag_part = dot3(w_split, x_split, NT)
    packed = jnp.concatenate([diag_part[:block // 2], diag_part[block // 2:]], axis=1)
    for h, part in enumerate(split(packed)):
        for q in range(pack):
            raw_snd[corr_n + h * pack + q] = part[q * CH:(q + 1) * CH]
    raw[0]()
    corr[1]()
    raw[1]()
    corr[2]()
    x_clean = x_half - dot3(split(take(corr_full) * inv_n), basis, NN)
    x_clean = split(x_clean)
    raw[2]()
    packed = jnp.concatenate([raw_full[corr_n + q] + raw_full[corr_n + pack + q] for q in range(pack)], axis=0) * inv_n
    diag_t = jnp.concatenate([packed[:, :block], packed[:, block:]], axis=0)
    w = w - (dot3(split(take(raw_full) * inv_n), basis, NN) + dot3(split(diag_t), x_clean, NN))
    image_half[...] = w
    pair2 = remote(image_half, image_other, pair_send.at[2], pair_recv.at[2], partner)
    pair2.start()
    zero = jnp.zeros((block, block), jnp.float32)
    square = jnp.concatenate([diag_t, zero], axis=1)
    square = jnp.concatenate([square, jnp.zeros_like(square)], axis=0).T
    diag_ref[...] = square[:block, :block]
    pair2.wait_recv()
    other = image_other[...]
    images = jnp.concatenate([jnp.where(first, w, other), jnp.where(first, other, w)], axis=1)
    image_ref[...] = images
    images = split(images)
    gram = dot3(images, images, NT)
    spot = r * C + c
    peers = R * C
    packed = jnp.concatenate([gram[:block // 2], gram[block // 2:]], axis=1)
    gram_rcv[spot] = packed

    def g_copy(i):
        p = lax.rem(spot + i, peers)
        return remote(gram_rcv.at[spot], gram_rcv.at[spot], g_send.at[i], g_recv.at[spot],
                      {"rows": p // C, "cols": p % C, "sub": s})

    loop(1, peers, lambda i: g_copy(i).start())

    def g_wait(i):
        p = lax.rem(spot + peers - i, peers)
        remote(gram_rcv.at[p], gram_rcv.at[p], g_send.at[i], g_recv.at[p], partner).wait_recv()

    loop(1, peers, g_wait)
    packed = jnp.sum(gram_rcv[...], axis=0) * inv_n
    gram = jnp.concatenate([packed[:, :block], packed[:, block:]], axis=0)

    gram_ref[...] = gram
    pair0.wait_send()
    pair1.wait_send()
    pair2.wait_send()

    def sent(i):
        x_copy(i).wait_send()
        p_copy(i, 0).wait_send()
        p_copy(i, 1).wait_send()

    loop(1, R, sent)
    corr[3]()
    raw[3]()
    loop(1, peers, lambda i: g_copy(i).wait_send())


def finish_kernel(image_ref, diag_in, gram_ref, new_ref, diag_ref, coup_ref):
    block = gram_ref.shape[0]
    row_id = lax.broadcasted_iota(jnp.int32, (block, block), 0)
    col_id = lax.broadcasted_iota(jnp.int32, (block, block), 1)
    eye = jnp.where(row_id == col_id, 1.0, 0.0)
    full = eliminate(jnp.concatenate([gram_ref[...], eye], axis=1), block)
    coup_ref[0] = jnp.where(col_id >= row_id, full[:, :block], 0.0)
    diag_ref[0] = diag_in[...]
    inverse = split(jnp.where(col_id <= row_id, full[:, block:], 0.0))
    new_ref[0] = dot3(inverse, split(image_ref[...]), NN)


def solution(mesh):
    R, C, S = mesh.shape["rows"], mesh.shape["cols"], mesh.shape["sub"]
    n = R * C * S

    def local(index, tiles, onsite, start, previous, coupling, stored):
        rows, block = start.shape
        tile = tiles.shape[1]
        assert rows == tile and S == 2 and 2 * block == LANES
        half = rows // 2
        mine = stored.shape[0] * block
        corr_n = (S * mine // LANES) * (block // CH)
        raw_n = corr_n + 2 * block * block // (CH * LANES)
        f32, bf16 = jnp.float32, jnp.bfloat16
        dma = pltpu.SemaphoreType.DMA

        def ring(nch, kind):
            slots = -(-nch // n)
            return [
                pltpu.VMEM((nch, CH, LANES), kind),
                pltpu.VMEM((slots, n, CH, LANES), kind),
                pltpu.VMEM((nch, CH, LANES), f32),
            ]

        def ring_sems(nch):
            slots = -(-nch // n)
            return [dma((nch,)), dma((slots, n)), dma((slots, n)), dma((nch,))]

        vmem = pl.BlockSpec(memory_space=pltpu.VMEM)
        hbm = pl.BlockSpec(memory_space=pl.ANY)
        image, diagonal, gram = pl.pallas_call(
            functools.partial(kernel, (R, C, S)),
            out_shape=(
                jax.ShapeDtypeStruct((block, rows), f32),
                jax.ShapeDtypeStruct((block, block), f32),
                jax.ShapeDtypeStruct((block, block), f32),
            ),
            in_specs=[pl.BlockSpec(memory_space=pltpu.SMEM), hbm, vmem, hbm, hbm, vmem, hbm],
            out_specs=(vmem, vmem, vmem),
            scratch_shapes=[
                pltpu.VMEM(tiles.shape, tiles.dtype),
                pltpu.VMEM((block, rows), f32),
                pltpu.VMEM((block, rows), f32),
                pltpu.VMEM((mine // block, block, rows), f32),
                dma((4,)),
                pltpu.VMEM((R, block, rows), bf16),
                pltpu.VMEM((R, S, block, half), bf16),
                pltpu.VMEM((R, S, block, half), bf16),
                pltpu.VMEM((block, half), f32),
                pltpu.VMEM((block, half), f32),
                pltpu.VMEM((mine // block, block, half), f32),
                *ring(corr_n, f32),
                *ring(raw_n, bf16),
                pltpu.VMEM((block, half), f32),
                pltpu.VMEM((block, half), f32),
                pltpu.VMEM((R * C, block // 2, LANES), f32),
                dma((R,)), dma((R,)), dma((R, S)), dma((R, S)), dma((3,)), dma((3,)),
                *ring_sems(corr_n),
                *ring_sems(raw_n),
                dma((R * C,)), dma((R * C,)),
            ],
            compiler_params=pltpu.CompilerParams(collective_id=0, has_side_effects=True),
        )(index, tiles, onsite.reshape(1, rows), start.T, previous.T, coupling, stored.transpose(0, 2, 1))
        new, diagonal, upper = pl.pallas_call(
            finish_kernel,
            out_shape=(
                jax.ShapeDtypeStruct((1, block, rows), f32),
                jax.ShapeDtypeStruct((1, block, block), f32),
                jax.ShapeDtypeStruct((1, block, block), f32),
            ),
            in_specs=[vmem] * 3,
            out_specs=(vmem, vmem, vmem),
        )(image, diagonal, gram)
        return new.transpose(0, 2, 1), diagonal, upper

    return jax.shard_map(
        local,
        mesh=mesh,
        in_specs=(
            P(("groups", "rows", "cols", "sub"), None),
            P(("groups", "rows", "cols", "sub"), None, None),
            P(("groups", "rows", "cols")),
            P(("groups", "rows", "cols"), None),
            P(("groups", "rows", "cols"), None),
            P("groups", None),
            P("sub", ("groups", "rows", "cols"), None),
        ),
        out_specs=(
            P(None, ("groups", "rows", "cols"), None),
            P(None, "groups", None),
            P(None, "groups", None),
        ),
        check_vma=False,
    )
```
